32 devices in a mesh: member: 4 (over y, x), lat: 8 (over z, core).
Axes of the slice: x: 2, y: 2, z: 4, core: 2. Of those that a mesh axis runs over, the one named last changes fastest.
Arguments:
- state: bfloat16 [4, 64, 720, 128], P('member', 'lat'), may hold values from -6 to 6
- conv_weight: bfloat16 [9, 128, 128], replicated, may hold values from -0.1875 to 0.1875
- legendre: bfloat16 [64, 64, 64], P('lat'), may hold values from -0.75 to 0.75
- quad_weight: float32 [64], replicated, may hold values from 0.5 to 2
- spectral_gain: float32 [2, 64, 128], replicated, may hold values from -4 to 4
- project_weight: float32 [128, 16], replicated, may hold values from -0.5 to 0.5
- target: bfloat16 [16, 64, 720], P(None, 'lat'), may hold values from -10 to 10
Outputs:
- field_grad: float32 [4, 16, 64, 720], P('member', None, 'lat')
The draws below stay inside these ranges and needn't reach their ends.
All inputs are finite; a program needn't handle non-finite values.
Results may differ from the reference program's by a relative error of at most 0.0088.
Values may be sent and summed in bfloat16 or wider, within the bound.
A program may use at most 64 MiB of HBM per device.

```python
import math
import jax
import jax.numpy as jnp
from jax import lax

NLON = 720
C = 128
FIELDS = 16
MODES = 64
NLAT = 64
MEMBERS = 4


def level_of(key, shape, pieces, low, high):
    loudness = 1.0
    for axis_at, parts in pieces:
        heights = jax.random.uniform(jax.random.fold_in(jax.random.fold_in(key, 6), axis_at), (parts,), jnp.float32, low / len(pieces), high / len(pieces))
        loudness = loudness * jnp.repeat(jnp.exp(heights), shape[axis_at] // parts).reshape((-1,) + (1,) * (len(shape) - 1 - axis_at))
    return loudness


def gaussian(key, shape, width, bound, shards=(), kind=jnp.bfloat16):
    result = jax.random.normal(key, shape, jnp.float32) * width
    if len(shards) > 0:
        result = level_of(key, shape, shards, -0.22, 0.18) * result
    return jnp.clip(result, min=-bound, max=bound).astype(kind)


def setup_inputs(seed: int = 0) -> dict:
    keys = jax.random.split(jax.random.key(seed), 8)
    return {
        "state": gaussian(keys[0], (MEMBERS, NLAT, NLON, C), 1.0, 6.0, ((0, 4), (1, 8))),
        "conv_weight": gaussian(keys[1], (9, C, C), (9 * C) ** -0.5, 0.1875),
        "legendre": gaussian(keys[2], (MODES, MODES, NLAT), NLAT ** -0.5, 0.75, ((0, 8),)),
        "quad_weight": jnp.clip(jnp.exp(jax.random.uniform(keys[3], (NLAT,), jnp.float32, math.log(0.5), math.log(2.0))), 0.5, 2.0),
        "spectral_gain": gaussian(keys[4], (2, MODES, C), 1.0, 4.0, (), jnp.float32),
        "project_weight": gaussian(keys[5], (C, FIELDS), C ** -0.5, 0.5, (), jnp.float32),
        "target": gaussian(keys[6], (FIELDS, NLAT, NLON), 2.0, 10.0, ((1, 8),)),
    }


def dft_table(nlon, modes):
    lon = jnp.arange(nlon, dtype=jnp.int32)
    wave = jnp.arange(modes, dtype=jnp.int32)
    phase = lon[:, None] * wave[None, :] % nlon
    angle = phase.astype(jnp.float32) * (2.0 * jnp.pi / nlon)
    table = jnp.concatenate([jnp.cos(angle), -jnp.sin(angle)], axis=1) / jnp.sqrt(jnp.float32(nlon))
    return table.astype(jnp.bfloat16)

def smooth(diff):
    return diff / jnp.sqrt(diff * diff + 0.25)

def reference(state, conv_weight, legendre, quad_weight, spectral_gain, project_weight, target):
    table = dft_table(NLON, MODES).astype(jnp.float32)
    wtable = (legendre.astype(jnp.float32) * quad_weight[None, None, :]).astype(jnp.bfloat16).astype(jnp.float32)
    legend = legendre.astype(jnp.float32)
    weights = conv_weight.astype(jnp.float32)
    gain_re = spectral_gain[0]
    gain_im = spectral_gain[1]

    def member_field(field):
        padded = jnp.pad(field, ((4, 4), (0, 0), (0, 0))).astype(jnp.float32)
        conv = jnp.zeros((NLAT, NLON, C), jnp.float32)
        for shift in range(9):
            conv = conv + jnp.einsum('anc,cd->and', padded[shift:shift + NLAT], weights[shift])
        mixed = (field.astype(jnp.float32) + jax.nn.silu(conv)).astype(jnp.bfloat16)
        spectrum = jnp.einsum('anc,nk->akc', mixed.astype(jnp.float32), table).astype(jnp.bfloat16)
        spectrum = spectrum.reshape(NLAT, 2, MODES, C).astype(jnp.float32)
        coef = jnp.einsum('mla,armc->mlrc', wtable, spectrum)
        real_part = coef[:, :, 0] * gain_re[None] - coef[:, :, 1] * gain_im[None]
        imag_part = coef[:, :, 0] * gain_im[None] + coef[:, :, 1] * gain_re[None]
        filtered = jnp.stack([real_part, imag_part], axis=2).astype(jnp.bfloat16).astype(jnp.float32)
        back = jnp.einsum('mla,mlrc->armc', legend, filtered).astype(jnp.bfloat16)
        back = back.reshape(NLAT, 2 * MODES, C).astype(jnp.float32)
        synth = jnp.einsum('akc,nk->anc', back, table)
        total = mixed.astype(jnp.float32) + synth
        projected = jnp.einsum('anc,cf->fan', total, project_weight, precision=lax.Precision.HIGHEST)
        return projected.astype(jnp.bfloat16)
    projected = lax.map(member_field, state).astype(jnp.float32)
    observed = target.astype(jnp.float32)

    def member_grad(own):
        pair = lax.optimization_barrier(jnp.sum(smooth(own[None] - projected), axis=0))
        return smooth(own - observed) - pair / (MEMBERS - 1)
    return lax.map(member_grad, projected)
```

```python
import jax
import jax.numpy as jnp
from jax import lax
from jax.sharding import PartitionSpec as P


def with_halo(block, sides, width):
    for axis, dim in sides:
        count = lax.axis_size(axis)
        forward = [(i, i + 1) for i in range(count - 1)]
        backward = [(target, source) for source, target in forward]
        low = lax.ppermute(
            lax.slice_in_dim(block, block.shape[dim] - width, None, axis=dim), axis, forward
        )
        high = lax.ppermute(lax.slice_in_dim(block, 0, width, axis=dim), axis, backward)
        block = jnp.concatenate([low, block, high], axis=dim)
    return block


def dft_table(nlon, modes):
    lon = jnp.arange(nlon, dtype=jnp.int32)
    wave = jnp.arange(modes, dtype=jnp.int32)
    phase = lon[:, None] * wave[None, :] % nlon
    angle = phase.astype(jnp.float32) * (2.0 * jnp.pi / nlon)
    table = jnp.concatenate([jnp.cos(angle), -jnp.sin(angle)], axis=1) / jnp.sqrt(jnp.float32(nlon))
    return table.astype(jnp.bfloat16)


def smooth(diff):
    return diff / jnp.sqrt(diff * diff + 0.25)


def local(state, conv_weight, legendre, quad_weight, spectral_gain, project_weight, target):
    field = state[0]
    lat_rows, nlon, chans = field.shape
    modes = legendre.shape[1]
    padded = with_halo(field, (("lat", 0),), 4)
    conv = lax.conv_general_dilated(
        padded,
        conv_weight,
        window_strides=(1,),
        padding="VALID",
        dimension_numbers=("WNC", "WIO", "WNC"),
        preferred_element_type=jnp.float32,
    )
    mixed = (field.astype(jnp.float32) + jax.nn.silu(conv)).astype(jnp.bfloat16)
    table = dft_table(nlon, modes)
    spectrum = jnp.einsum("anc,nk->akc", mixed, table, preferred_element_type=jnp.float32).astype(
        jnp.bfloat16
    )
    spectrum = spectrum.reshape(lat_rows, 2, modes, chans)
    banded = lax.all_to_all(spectrum, "lat", split_axis=2, concat_axis=0, tiled=True)
    wtable = (legendre.astype(jnp.float32) * quad_weight[None, None, :]).astype(jnp.bfloat16)
    coef = jnp.einsum("mla,armc->mlrc", wtable, banded, preferred_element_type=jnp.float32)
    gain_re = spectral_gain[0]
    gain_im = spectral_gain[1]
    real_part = coef[:, :, 0] * gain_re[None] - coef[:, :, 1] * gain_im[None]
    imag_part = coef[:, :, 0] * gain_im[None] + coef[:, :, 1] * gain_re[None]
    filtered = jnp.stack([real_part, imag_part], axis=2).astype(jnp.bfloat16)
    back = jnp.einsum(
        "mla,mlrc->armc", legendre, filtered, preferred_element_type=jnp.float32
    ).astype(jnp.bfloat16)
    high = lax.reduce_precision(project_weight, 8, 7)
    weight = jnp.concatenate([high, project_weight - high], axis=1).astype(jnp.bfloat16)
    fields = project_weight.shape[1]
    both = jnp.einsum("armc,cg->armg", back, weight, preferred_element_type=jnp.float32)
    narrow = (both[..., :fields] + both[..., fields:]).astype(jnp.bfloat16)
    rowwise = lax.all_to_all(narrow, "lat", split_axis=0, concat_axis=2, tiled=True)
    synth = jnp.einsum(
        "akf,nk->fan",
        rowwise.reshape(lat_rows, 2 * modes, fields),
        table,
        preferred_element_type=jnp.float32,
    )
    direct = jnp.einsum("anc,cg->gan", mixed, weight, preferred_element_type=jnp.float32)
    projected = (direct[:fields] + direct[fields:] + synth).astype(jnp.bfloat16)
    members = lax.axis_size("member")
    own = projected.astype(jnp.float32)
    pair = jnp.sum(
        smooth(
            own[None]
            - lax.all_gather(projected[None], "member", axis=0, tiled=True).astype(jnp.float32)
        ),
        axis=0,
    )
    grads = smooth(own - target.astype(jnp.float32)) - pair / (members - 1)
    return grads[None]


def solution(mesh):
    return jax.shard_map(
        local,
        mesh=mesh,
        in_specs=(
            P("member", "lat", None, None),
            P(),
            P("lat", None, None),
            P(),
            P(),
            P(),
            P(None, "lat", None),
        ),
        out_specs=P("member", None, "lat", None),
        check_vma=False,
    )
```
